1024 devices in a mesh: dp: 64 (over x, y, core), tensor: 16 (over z).
Axes of the slice: x: 4, y: 8, z: 16, core: 2. Of those that a mesh axis runs over, the one named last changes fastest.
Arguments:
- tokens: bfloat16 [8192, 6144], P('dp', 'tensor'), may hold values from -6 to 6
- expert_ids: int32 [8192, 2], P('dp'), may hold values from 0 to 63, all different within a row; in each aligned block of 128 rows (0 to 127, 128 to 255, ...) at most 5 rows name the same one
- combine: float32 [8192, 2], P('dp'), may hold values from 0.2 to 1
- up_weight: bfloat16 [64, 6144, 2048], P('dp', None, 'tensor'), may hold values from -0.078125 to 0.078125
- down_weight: bfloat16 [64, 2048, 6144], P('dp', 'tensor'), may hold values from -0.1875 to 0.1875
Outputs:
- mixed: bfloat16 [8192, 6144], P('dp', 'tensor')
The draws below stay inside these ranges and needn't reach their ends.
Inputs may be any that keep to these rules, and one draw needn't show every extreme that they name: `expert_ids`: each token names 2 different experts. Among the 128 tokens of one index of dp, no expert is named more than 5 times, a bound that some block reaches.
All inputs are finite; a program needn't handle non-finite values.
Results may differ from the reference program's by a relative error of at most 0.019.
Values may be sent and summed in bfloat16 or wider, within the bound.
No kernel may reach another device: no remote copies, remote signals or barrier semaphores. Data moves between devices by JAX's collectives and lax.ppermute only.
A program may use at most 32 MiB of HBM per device.

```python
import math
import jax
import jax.numpy as jnp
import numpy as np
from jax import lax

D = 6144
FF = 2048
TOP = 2
TOK_DEV = 128
EXPERTS = 64
CAP = 5
TOKENS = 8192
N_DP = 64
N_TENSOR = 16


def with_spikes(result, rng, source, target, parts, factor):
    owner, partner = [(jnp.arange(result.shape[position]) // (result.shape[position] // parts)).reshape([-1 if axis == position else 1 for axis in range(result.ndim)]) for position in (source, target)]
    chosen = jax.random.permutation(rng, parts)[partner]
    strong = (owner == chosen) | (owner == (partner + parts // 2) % parts)
    return jnp.where(strong, factor * result, result)


def levels(rng, dims, shards, low, high):
    level = 1.0
    for position, shards_of in shards:
        steps = jax.random.uniform(jax.random.fold_in(jax.random.fold_in(rng, 6), position), (shards_of,), jnp.float32, low / len(shards), high / len(shards))
        level = level * jnp.repeat(jnp.exp(steps), dims[position] // shards_of).reshape((-1,) + (1,) * (len(dims) - 1 - position))
    return level


def shared_out(rng, own, number, rows, count, top, limit, skew):
    ranking = jax.random.permutation(rng, count)
    heavy_load, ordinary = load_shares(count, rows * top, limit, skew, True), load_shares(count, rows * top, limit, skew, False)
    places = jnp.arange(count)

    def named(tallies, offset_by):
        used = int((tallies > 0).sum())
        fixed = max(1, used // 4)
        moved = fixed + (places - fixed + offset_by * (used - fixed)) % max(1, count - fixed)
        return jnp.zeros((count,), jnp.int32).at[ranking[jnp.where(places < fixed, places, moved)]].set(jnp.asarray(tallies, jnp.int32))

    tallies = jnp.where(number % 4 == 0, named(heavy_load, number // 4), named(ordinary, number - number // 4 - 1))
    mixed = jax.random.permutation(jax.random.fold_in(own, 3), count)
    donor, receiver = mixed[0:count // 2 * 2:2], mixed[1:count // 2 * 2:2]
    room = jnp.minimum(tallies[donor] - 1, limit - tallies[receiver]) // 2
    room = jnp.where((donor == ranking[0]) | (receiver == ranking[0]) | (tallies[receiver] == 0), 0, jnp.maximum(room, 0))
    moved = jax.random.randint(jax.random.fold_in(own, 4), (count // 2,), 0, 1 << 20) % (room + 1)
    tallies = tallies.at[donor].add(-moved).at[receiver].add(moved)
    members = jnp.searchsorted(jnp.cumsum(tallies), jnp.arange(rows * top), side="right").astype(jnp.int32)
    listing = members.reshape(top, rows).T
    listing = listing[jax.random.permutation(jax.random.fold_in(own, 1), rows)]
    offset_by = jax.random.randint(jax.random.fold_in(own, 2), (rows, 1), 0, top)
    return jnp.take_along_axis(listing, (jnp.arange(top)[None, :] + offset_by) % top, axis=1)


def load_shares(amount, total, most, slope, full):
    weights = [(1 << 20) // math.isqrt(grade ** slope) + 1 for grade in range(1, amount + 1)]
    largest = most if full else min(most, max(-(-total // amount), total * weights[0] // sum(weights)))
    least = 1 if total - largest >= amount - 1 else 0
    given, rest = [largest] + [least] * (amount - 1), total - largest - least * (amount - 1)
    while rest > 0:
        free = [i for i in range(1, amount) if given[i] < largest] or [i for i in range(1, amount) if given[i] < most]
        mass, budget = sum([weights[i] for i in free]), rest
        for i in free:
            addition = min(most - given[i], max(1, budget * weights[i] // mass), rest)
            given[i] = given[i] + addition
            rest = rest - addition
    return np.array(given)


def centred(key, shape, width, bound, shards=(), kind=jnp.bfloat16):
    level = levels(key, shape, shards, -0.22, 0.18) if shards else 1.0
    entries = jax.random.normal(key, shape, jnp.float32) * width * level
    return jnp.minimum(jnp.maximum(entries, -bound), bound).astype(kind)


def noise_with(stream_key, dims, width, limit, pieces, heavy, kind=jnp.bfloat16):
    values = width * jax.random.normal(stream_key, dims, jnp.float32)
    if pieces:
        values = values * levels(stream_key, dims, pieces, -0.22, 0.18)
    return jnp.clip(with_spikes(values, jax.random.fold_in(stream_key, 3), *heavy), -limit, limit).astype(kind)


def setup_inputs(seed: int = 0) -> dict:
    seeds = jax.random.split(jax.random.key(seed), 6)
    tokens = centred(seeds[0], (TOKENS, D), 1.0, 6.0, ((0, 64), (1, 16)))
    expert_ids_keys = jax.random.split(jax.random.fold_in(seeds[1], 1), TOKENS // TOK_DEV)
    expert_ids_turns = jax.random.permutation(jax.random.fold_in(seeds[1], 3), TOKENS // TOK_DEV)
    expert_ids = jax.vmap(lambda own, number: shared_out(jax.random.fold_in(seeds[1], 2), own, number, TOK_DEV, EXPERTS, TOP, CAP, 2))(expert_ids_keys, expert_ids_turns).reshape((TOKENS, TOP))
    combine = jnp.clip(0.2 + 0.8 * jax.random.uniform(seeds[2], (TOKENS, TOP), jnp.float32) ** levels(seeds[2], (TOKENS, TOP), ((0, 64),), -0.2, 0.2), 0.2, 1.0)
    up_weight = centred(seeds[3], (EXPERTS, D, FF), D ** -0.5, 0.078125, ((0, 64), (2, 16)))
    down_weight = noise_with(seeds[4], (EXPERTS, FF, D), FF ** -0.5, 0.1875, ((0, 64), (1, 16)), (1, 2, 16, 2.0))
    return dict(tokens=tokens, expert_ids=expert_ids, combine=combine, up_weight=up_weight, down_weight=down_weight)


def slot_rows(expert_ids):
    ids = expert_ids.reshape(N_DP, TOK_DEV * TOP)
    onehot = (ids[:, :, None] == jnp.arange(EXPERTS, dtype=jnp.int32)[None, None, :]).astype(jnp.int32)
    earlier = jnp.cumsum(onehot, axis=1) - onehot
    slots = jnp.sum(earlier * onehot, axis=2).astype(jnp.int32)
    source = jnp.arange(N_DP, dtype=jnp.int32)[:, None]
    rows = (source * CAP + slots).astype(jnp.int32)
    return ids.reshape(-1), rows.reshape(-1)


def reference(tokens, expert_ids, combine, up_weight, down_weight):
    ids, rows = slot_rows(expert_ids)
    total_rows = N_DP * CAP
    share = FF // N_TENSOR
    token_of = (jnp.arange(TOKENS * TOP, dtype=jnp.int32) // TOP).astype(jnp.int32)
    repeated = tokens[token_of]

    def run_expert(packed):
        index, up_w, down_w = packed
        target = jnp.where(ids == index, rows, total_rows).astype(jnp.int32)
        buffer = jnp.zeros((total_rows, D), jnp.bfloat16).at[target].set(repeated, mode="drop")
        hidden = jax.nn.silu(jnp.dot(buffer, up_w, preferred_element_type=jnp.float32)).astype(jnp.bfloat16)
        blocks = jnp.einsum("rtf,tfd->trd", hidden.reshape(total_rows, N_TENSOR, share).astype(jnp.float32),
                            down_w.reshape(N_TENSOR, share, D).astype(jnp.float32))
        rounded = lax.optimization_barrier(blocks.astype(jnp.bfloat16))
        return jnp.sum(rounded.astype(jnp.float32), axis=0).astype(jnp.bfloat16)

    outputs = lax.map(run_expert, (jnp.arange(EXPERTS, dtype=jnp.int32), up_weight, down_weight))
    picked = outputs[ids, rows].astype(jnp.float32).reshape(TOKENS, TOP, D)
    mixed = jnp.sum(picked * combine[:, :, None], axis=1)
    return mixed.astype(jnp.bfloat16)
```

```python
import jax
import jax.numpy as jnp
from jax import lax
from jax.experimental.layout import Layout, with_layout_constraint
from jax.sharding import Mesh
from jax.sharding import PartitionSpec as P


LANES = 128
SCALE = 8192.0


def swap(value, axis, step):
    size = lax.axis_size(axis)
    return lax.ppermute(value, axis, [(i, i ^ step) for i in range(size)])


def shift(value, axis, step):
    size = lax.axis_size(axis)
    return lax.ppermute(value, axis, [(i, (i + step) % size) for i in range(size)])


def on_device(tokens, expert_ids, combine, up_weight, down_weight):
    tok_rows, feat = tokens.shape
    experts = lax.axis_size("dp")
    high, low = lax.axis_size("hi"), lax.axis_size("lo")
    capacity = 5 * tok_rows // (2 * experts)
    picks = expert_ids.shape[1]
    tiles = feat // LANES
    packed_rows = -(-(capacity * tiles) // 16) * 16
    row_count = experts * capacity

    down_local = down_weight[0]
    mine, group = lax.axis_index("lo"), lax.axis_index("hi")

    def share(step):
        cuts = []
        for turn in range(high):
            owner = (group + turn) % high * low + (mine ^ step)
            cuts.append(lax.dynamic_slice_in_dim(down_local, owner * feat, feat, axis=1))
        block = jnp.concatenate(cuts, axis=1)
        return with_layout_constraint(block, Layout(major_to_minor=(0, 1)))

    down_parts = [share(0)]
    for step in range(1, low):
        down_parts.append(swap(share(step), "lo", step))

    token = jnp.arange(tok_rows, dtype=jnp.int32)
    before = token[:, None] < token[None, :]
    slots = []
    for pick in range(picks):
        same = jnp.zeros((tok_rows, tok_rows), jnp.int32)
        for other in range(picks):
            same = same + (expert_ids[:, other][:, None] == expert_ids[:, pick][None, :])
        slots.append(jnp.sum(jnp.where(before, same, 0), axis=0))
    slots = jnp.stack(slots, axis=1)
    place = expert_ids * packed_rows + slots
    spots = jnp.arange(experts * packed_rows, dtype=jnp.int32)[None, :]

    def chosen(pick, tile):
        return place[:, pick][:, None] + tile * capacity == spots

    outgoing = jnp.zeros((experts * packed_rows, LANES), jnp.float32)
    for tile in range(tiles):
        both = (chosen(0, tile) | chosen(1, tile)).astype(jnp.bfloat16)
        outgoing = outgoing + jnp.einsum(
            "ts,tf->sf", both, tokens[:, tile * LANES : (tile + 1) * LANES],
            preferred_element_type=jnp.float32,
        )
    outgoing = outgoing.astype(jnp.bfloat16).reshape(experts, packed_rows, LANES)
    received = lax.all_to_all(outgoing, "dp", split_axis=0, concat_axis=0, tiled=True)
    received = received.reshape(experts * packed_rows, LANES)

    rows = jnp.arange(row_count, dtype=jnp.int32)
    row_spot = (rows // capacity) * packed_rows + rows % capacity

    def unpacker(tile):
        return (row_spot[:, None] + tile * capacity == spots).astype(jnp.bfloat16)

    flat_rows = jnp.concatenate(
        [
            jnp.dot(unpacker(tile), received, preferred_element_type=jnp.float32)
            for tile in range(tiles)
        ],
        axis=1,
    )
    scaled = (flat_rows * SCALE).astype(jnp.float16)
    gathered = lax.all_gather(scaled, ("hi", "lo"), axis=1, tiled=True)
    accum = jnp.dot(gathered.astype(jnp.bfloat16), up_weight[0], preferred_element_type=jnp.float32)
    hidden = jax.nn.silu(accum * (1.0 / SCALE)).astype(jnp.bfloat16)
    pieces = [hidden] + [swap(hidden, "lo", step) for step in range(1, low)]
    hidden = jnp.concatenate(pieces, axis=1)
    down_mine = jnp.concatenate(down_parts, axis=0)
    part = jnp.dot(hidden, down_mine, preferred_element_type=jnp.float32)

    keep, ahead, across, behind = [part[:, k * feat : (k + 1) * feat] for k in range(high)]
    half = row_count // 2
    across = across.astype(jnp.bfloat16)
    from_behind = shift(across[:half], "hi", 1)
    from_ahead = shift(across[half:], "hi", -1)
    ahead = jnp.concatenate([ahead[:half] + from_behind.astype(jnp.float32), ahead[half:]], axis=0)
    behind = jnp.concatenate([behind[:half], behind[half:] + from_ahead.astype(jnp.float32)], axis=0)
    one = shift(ahead.astype(jnp.bfloat16), "hi", 1)
    two = shift(behind.astype(jnp.bfloat16), "hi", -1)
    result = keep + one.astype(jnp.float32) + two.astype(jnp.float32)
    result = result.astype(jnp.bfloat16)

    packed = jnp.zeros((experts * packed_rows, LANES), jnp.float32)
    for tile in range(tiles):
        packed = packed + jnp.einsum(
            "rs,rf->sf", unpacker(tile), result[:, tile * LANES : (tile + 1) * LANES],
            preferred_element_type=jnp.float32,
        )
    packed = packed.astype(jnp.bfloat16).reshape(experts, packed_rows, LANES)
    returned = lax.all_to_all(packed, "dp", split_axis=0, concat_axis=0, tiled=True)
    returned = returned.reshape(experts * packed_rows, LANES)
    columns = []
    for tile in range(tiles):
        total = 0.0
        for pick in range(picks):
            one_hot = chosen(pick, tile).astype(jnp.bfloat16)
            row = jnp.dot(one_hot, returned, preferred_element_type=jnp.float32)
            total = total + row * combine[:, pick][:, None]
        columns.append(total)
    return jnp.concatenate(columns, axis=1).astype(jnp.bfloat16)


def solution(mesh):
    shape = mesh.devices.shape
    low = 4
    split = Mesh(mesh.devices.reshape(shape[0], shape[1] // low, low), ("dp", "hi", "lo"))
    tensor = ("hi", "lo")
    placed = (
        P("dp", tensor),
        P("dp", None),
        P("dp", None),
        P("dp", None, tensor),
        P("dp", tensor, None),
    )
    return jax.shard_map(
        on_device, mesh=split, in_specs=placed, out_specs=P("dp", tensor), check_vma=False
    )
```

```python
import jax
import jax.numpy as jnp
from jax import lax
from jax.experimental.layout import Layout, with_layout_constraint
from jax.sharding import Mesh
from jax.sharding import PartitionSpec as P


LANES = 128
SCALE = 8192.0


def swap(value, axis, step):
    size = lax.axis_size(axis)
    return lax.ppermute(value, axis, [(i, i ^ step) for i in range(size)])


def shift(value, axis, step):
    size = lax.axis_size(axis)
    return lax.ppermute(value, axis, [(i, (i + step) % size) for i in range(size)])


def on_device(tokens, expert_ids, combine, up_weight, down_weight):
    tok_rows, feat = tokens.shape
    experts = lax.axis_size("dp")
    high, low = lax.axis_size("hi"), lax.axis_size("lo")
    capacity = 5 * tok_rows // (2 * experts)
    picks = expert_ids.shape[1]
    tiles = feat // LANES
    packed_rows = -(-(capacity * tiles) // 16) * 16
    row_count = experts * capacity

    down_local = down_weight[0]
    mine, group = lax.axis_index("lo"), lax.axis_index("hi")

    def share(step):
        cuts = []
        for turn in range(high):
            owner = (group + turn) % high * low + (mine ^ step)
            cuts.append(lax.dynamic_slice_in_dim(down_local, owner * feat, feat, axis=1))
        block = jnp.concatenate(cuts, axis=1)
        return with_layout_constraint(block, Layout(major_to_minor=(0, 1)))

    down_parts = [share(0)]
    for step in range(1, low):
        down_parts.append(swap(share(step), "lo", step))

    token = jnp.arange(tok_rows, dtype=jnp.int32)
    before = token[:, None] < token[None, :]
    slots = []
    for pick in range(picks):
        same = jnp.zeros((tok_rows, tok_rows), jnp.int32)
        for other in range(picks):
            same = same + (expert_ids[:, other][:, None] == expert_ids[:, pick][None, :])
        slots.append(jnp.sum(jnp.where(before, same, 0), axis=0))
    slots = jnp.stack(slots, axis=1)
    place = expert_ids * packed_rows + slots
    spots = jnp.arange(experts * packed_rows, dtype=jnp.int32)[None, :]

    def chosen(pick, tile):
        return place[:, pick][:, None] + tile * capacity == spots

    both = jnp.concatenate([chosen(0, tile) | chosen(1, tile) for tile in range(tiles)], axis=0)
    stacked = jnp.concatenate(
        [tokens[:, tile * LANES : (tile + 1) * LANES] for tile in range(tiles)], axis=0
    )
    outgoing = jnp.einsum(
        "ts,tf->sf", both.astype(jnp.bfloat16), stacked, preferred_element_type=jnp.float32
    )
    outgoing = outgoing.astype(jnp.bfloat16).reshape(experts, packed_rows, LANES)
    received = lax.all_to_all(outgoing, "dp", split_axis=0, concat_axis=0, tiled=True)
    received = received.reshape(experts * packed_rows, LANES)

    rows = jnp.arange(row_count, dtype=jnp.int32)
    row_spot = (rows // capacity) * packed_rows + rows % capacity

    row_spots = jnp.concatenate([row_spot + tile * capacity for tile in range(tiles)])
    unpacker = (row_spots[:, None] == spots).astype(jnp.bfloat16)
    flat_rows = jnp.dot(unpacker, received, preferred_element_type=jnp.float32)
    flat_rows = jnp.concatenate(
        [flat_rows[tile * row_count : (tile + 1) * row_count] for tile in range(tiles)], axis=1
    )
    scaled = (flat_rows * SCALE).astype(jnp.float16)
    gathered = lax.all_gather(scaled, ("hi", "lo"), axis=1, tiled=True)
    accum = jnp.dot(gathered.astype(jnp.bfloat16), up_weight[0], preferred_element_type=jnp.float32)
    hidden = jax.nn.silu(accum * (1.0 / SCALE)).astype(jnp.bfloat16)
    pieces = [hidden] + [swap(hidden, "lo", step) for step in range(1, low)]
    hidden = jnp.concatenate(pieces, axis=1)
    down_mine = jnp.concatenate(down_parts, axis=0)

    def block(k):
        columns = down_mine[:, k * feat : (k + 1) * feat]
        return jnp.dot(hidden, columns, preferred_element_type=jnp.float32)

    half = row_count // 2
    across = block(2).astype(jnp.bfloat16)
    far_one = shift(across[:half], "hi", 1)
    far_two = shift(across[half:], "hi", -1)
    ahead, behind = block(1), block(3)
    near_one = shift(ahead[half:].astype(jnp.bfloat16), "hi", 1)
    near_two = shift(behind[:half].astype(jnp.bfloat16), "hi", -1)
    keep = block(0)
    sum_one = shift((ahead[:half] + far_one.astype(jnp.float32)).astype(jnp.bfloat16), "hi", 1)
    sum_two = shift((behind[half:] + far_two.astype(jnp.float32)).astype(jnp.bfloat16), "hi", -1)
    upper = keep[:half] + near_two.astype(jnp.float32) + sum_one.astype(jnp.float32)
    lower = keep[half:] + near_one.astype(jnp.float32) + sum_two.astype(jnp.float32)
    result = jnp.concatenate([upper, lower], axis=0).astype(jnp.bfloat16)

    stacked = jnp.concatenate(
        [result[:, tile * LANES : (tile + 1) * LANES] for tile in range(tiles)], axis=0
    )
    spot = jnp.arange(experts * packed_rows, dtype=jnp.int32)
    within = spot % packed_rows
    source_row = within // capacity * row_count + spot // packed_rows * capacity + within % capacity
    source_row = jnp.where(within < tiles * capacity, source_row, -1)
    packer = source_row[:, None] == jnp.arange(tiles * row_count, dtype=jnp.int32)[None, :]
    packed = jnp.dot(packer.astype(jnp.bfloat16), stacked, preferred_element_type=jnp.float32)
    packed = packed.astype(jnp.bfloat16).reshape(experts, packed_rows, LANES)
    returned = lax.all_to_all(packed, "dp", split_axis=0, concat_axis=0, tiled=True)
    returned = returned.reshape(experts * packed_rows, LANES)
    spread = jnp.concatenate(
        [jnp.roll(returned, -tile * capacity, axis=0) for tile in range(tiles)], axis=1
    )
    total = 0.0
    for pick in range(picks):
        one_hot = chosen(pick, 0).astype(jnp.bfloat16)
        row = jnp.dot(one_hot, spread, preferred_element_type=jnp.float32)
        total = total + row * combine[:, pick][:, None]
    return with_layout_constraint(total.astype(jnp.bfloat16), Layout(major_to_minor=(0, 1)))


def solution(mesh):
    shape = mesh.devices.shape
    low = 4
    split = Mesh(mesh.devices.reshape(shape[0], shape[1] // low, low), ("dp", "hi", "lo"))
    tensor = ("hi", "lo")
    placed = (
        P("dp", tensor),
        P("dp", None),
        P("dp", None),
        P("dp", None, tensor),
        P("dp", tensor, None),
    )
    return jax.shard_map(
        on_device, mesh=split, in_specs=placed, out_specs=P("dp", tensor), check_vma=False
    )
```

```python
import jax
import jax.numpy as jnp
from jax import lax
from jax.experimental.layout import Layout, with_layout_constraint
from jax.sharding import Mesh
from jax.sharding import PartitionSpec as P


LANES = 128
SCALE = 8192.0


def swap(value, axis, step):
    size = lax.axis_size(axis)
    return lax.ppermute(value, axis, [(i, i ^ step) for i in range(size)])


def shift(value, axis, step):
    size = lax.axis_size(axis)
    return lax.ppermute(value, axis, [(i, (i + step) % size) for i in range(size)])


def on_device(tokens, expert_ids, combine, up_weight, down_weight):
    tok_rows, feat = tokens.shape
    experts = lax.axis_size("dp")
    high, low = lax.axis_size("hi"), lax.axis_size("lo")
    capacity = 5 * tok_rows // (2 * experts)
    picks = expert_ids.shape[1]
    tiles = feat // LANES
    packed_rows = -(-(capacity * tiles) // 16) * 16
    row_count = experts * capacity

    down_local = down_weight[0]
    mine, group = lax.axis_index("lo"), lax.axis_index("hi")

    def share(step):
        cuts = []
        for turn in range(high):
            owner = (group + turn) % high * low + (mine ^ step)
            cuts.append(lax.dynamic_slice_in_dim(down_local, owner * feat, feat, axis=1))
        block = jnp.concatenate(cuts, axis=1)
        return with_layout_constraint(block, Layout(major_to_minor=(0, 1)))

    down_parts = [share(0)]
    for step in range(1, low):
        down_parts.append(swap(share(step), "lo", step))

    token = jnp.arange(tok_rows, dtype=jnp.int32)
    before = token[:, None] < token[None, :]
    slots = []
    for pick in range(picks):
        same = jnp.zeros((tok_rows, tok_rows), jnp.int32)
        for other in range(picks):
            same = same + (expert_ids[:, other][:, None] == expert_ids[:, pick][None, :])
        slots.append(jnp.sum(jnp.where(before, same, 0), axis=0))
    slots = jnp.stack(slots, axis=1)
    place = expert_ids * packed_rows + slots
    spots = jnp.arange(experts * packed_rows, dtype=jnp.int32)[None, :]

    def chosen(pick, tile):
        return place[:, pick][:, None] + tile * capacity == spots

    both = jnp.concatenate([chosen(0, tile) | chosen(1, tile) for tile in range(tiles)], axis=0)
    stacked = jnp.concatenate(
        [tokens[:, tile * LANES : (tile + 1) * LANES] for tile in range(tiles)], axis=0
    )
    outgoing = jnp.einsum(
        "ts,tf->sf", both.astype(jnp.bfloat16), stacked, preferred_element_type=jnp.float32
    )
    outgoing = outgoing.astype(jnp.bfloat16).reshape(experts, packed_rows, LANES)
    received = lax.all_to_all(outgoing, "dp", split_axis=0, concat_axis=0, tiled=True)
    received = received.reshape(experts * packed_rows, LANES)

    rows = jnp.arange(row_count, dtype=jnp.int32)
    row_spot = (rows // capacity) * packed_rows + rows % capacity

    row_spots = jnp.concatenate([row_spot + tile * capacity for tile in range(tiles)])
    unpacker = (row_spots[:, None] == spots).astype(jnp.bfloat16)
    flat_rows = jnp.dot(unpacker, received, preferred_element_type=jnp.float32)
    flat_rows = jnp.concatenate(
        [flat_rows[tile * row_count : (tile + 1) * row_count] for tile in range(tiles)], axis=1
    )
    scaled = (flat_rows * SCALE).astype(jnp.float16)
    gathered = lax.all_gather(scaled, ("hi", "lo"), axis=1, tiled=True)
    accum = jnp.dot(gathered.astype(jnp.bfloat16), up_weight[0], preferred_element_type=jnp.float32)
    hidden = jax.nn.silu(accum * (1.0 / SCALE)).astype(jnp.bfloat16)
    pieces = [hidden] + [swap(hidden, "lo", step) for step in range(1, low)]
    hidden = jnp.concatenate(pieces, axis=1)
    down_mine = jnp.concatenate(down_parts, axis=0)

    half, reach = row_count // 2, high // 2
    halves = [hidden[:half], hidden[half:]]

    def cut(k, part):
        columns = down_mine[:, k % high * feat : (k % high + 1) * feat]
        return jnp.dot(halves[part], columns, preferred_element_type=jnp.float32)

    chains = [(0, 1, reach), (1, -1, reach), (1, 1, reach - 1), (0, -1, reach - 1)]
    arrived = [None] * len(chains)
    for distance in range(reach, 0, -1):
        for number, (part, way, length) in enumerate(chains):
            if distance <= length:
                value = cut(way * distance, part)
                if arrived[number] is not None:
                    value = value + arrived[number].astype(jnp.float32)
                arrived[number] = shift(value.astype(jnp.bfloat16), "hi", way)
    sums = []
    for part in range(2):
        value = cut(0, part)
        for number, chain in enumerate(chains):
            if chain[0] == part:
                value = value + arrived[number].astype(jnp.float32)
        sums.append(value)
    result = jnp.concatenate(sums, axis=0).astype(jnp.bfloat16)

    stacked = jnp.concatenate(
        [result[:, tile * LANES : (tile + 1) * LANES] for tile in range(tiles)], axis=0
    )
    spot = jnp.arange(experts * packed_rows, dtype=jnp.int32)
    within = spot % packed_rows
    source_row = within // capacity * row_count + spot // packed_rows * capacity + within % capacity
    source_row = jnp.where(within < tiles * capacity, source_row, -1)
    packer = source_row[:, None] == jnp.arange(tiles * row_count, dtype=jnp.int32)[None, :]
    packed = jnp.dot(packer.astype(jnp.bfloat16), stacked, preferred_element_type=jnp.float32)
    packed = packed.astype(jnp.bfloat16).reshape(experts, packed_rows, LANES)
    returned = lax.all_to_all(packed, "dp", split_axis=0, concat_axis=0, tiled=True)
    returned = returned.reshape(experts * packed_rows, LANES)
    spread = jnp.concatenate(
        [jnp.roll(returned, -tile * capacity, axis=0) for tile in range(tiles)], axis=1
    )
    total = 0.0
    for pick in range(picks):
        one_hot = chosen(pick, 0).astype(jnp.bfloat16)
        row = jnp.dot(one_hot, spread, preferred_element_type=jnp.float32)
        total = total + row * combine[:, pick][:, None]
    return with_layout_constraint(total.astype(jnp.bfloat16), Layout(major_to_minor=(0, 1)))


def solution(mesh):
    shape = mesh.devices.shape
    low = 2
    split = Mesh(mesh.devices.reshape(shape[0], shape[1] // low, low), ("dp", "hi", "lo"))
    tensor = ("hi", "lo")
    placed = (
        P("dp", tensor),
        P("dp", None),
        P("dp", None),
        P("dp", None, tensor),
        P("dp", tensor, None),
    )
    return jax.shard_map(
        on_device, mesh=split, in_specs=placed, out_specs=P("dp", tensor), check_vma=False
    )
```

```python
import jax
import jax.numpy as jnp
from jax import lax
from jax.experimental.layout import Layout, with_layout_constraint
from jax.sharding import PartitionSpec as P


LANES = 128
SCALE = 8192.0


GROUPS = 4


def shift(value, step):
    size = lax.axis_size("tensor")
    return lax.ppermute(value, "tensor", [(i, (i + step) % size) for i in range(size)])


def leap(value):
    size = lax.axis_size("tensor")
    pairs = [(i, (i + (2 if i % 2 else -2)) % size) for i in range(size)]
    return lax.ppermute(value, "tensor", pairs)


def on_device(tokens, expert_ids, combine, up_weight, down_weight):
    tok_rows, feat = tokens.shape
    experts = lax.axis_size("dp")
    places = lax.axis_size("tensor")
    stride = places // GROUPS
    capacity = 5 * tok_rows // (2 * experts)
    picks = expert_ids.shape[1]
    tiles = feat // LANES
    packed_rows = -(-(capacity * tiles) // 16) * 16
    row_count = experts * capacity

    down_local = down_weight[0]
    mine = lax.axis_index("tensor")

    down_late = lax.optimization_barrier(down_local)

    def share(source, move):
        cuts = []
        for turn in range(GROUPS):
            owner = (mine + move + turn * stride + places) % places
            cuts.append(lax.dynamic_slice_in_dim(source, owner * feat, feat, axis=1))
        block = jnp.concatenate(cuts, axis=1)
        return with_layout_constraint(block, Layout(major_to_minor=(0, 1)))

    leapt = leap(share(down_local, jnp.where(mine % 2 == 0, -2, 2)))
    down_parts = [share(down_late, 0)]
    down_parts += [shift(share(down_late, move), move) for move in (1, -1)]
    down_parts.append(leapt)

    token = jnp.arange(tok_rows, dtype=jnp.int32)
    before = token[:, None] < token[None, :]
    slots = []
    for pick in range(picks):
        same = jnp.zeros((tok_rows, tok_rows), jnp.int32)
        for other in range(picks):
            same = same + (expert_ids[:, other][:, None] == expert_ids[:, pick][None, :])
        slots.append(jnp.sum(jnp.where(before, same, 0), axis=0))
    slots = jnp.stack(slots, axis=1)
    place = expert_ids * packed_rows + slots
    spots = jnp.arange(experts * packed_rows, dtype=jnp.int32)[None, :]

    def chosen(pick, tile):
        return place[:, pick][:, None] + tile * capacity == spots

    both = jnp.concatenate([chosen(0, tile) | chosen(1, tile) for tile in range(tiles)], axis=0)
    stacked = jnp.concatenate(
        [tokens[:, tile * LANES : (tile + 1) * LANES] for tile in range(tiles)], axis=0
    )
    outgoing = jnp.einsum(
        "ts,tf->sf", both.astype(jnp.bfloat16), stacked, preferred_element_type=jnp.float32
    )
    outgoing = outgoing.astype(jnp.bfloat16).reshape(experts, packed_rows, LANES)
    received = lax.all_to_all(outgoing, "dp", split_axis=0, concat_axis=0, tiled=True)
    received = received.reshape(experts * packed_rows, LANES)

    rows = jnp.arange(row_count, dtype=jnp.int32)
    row_spot = (rows // capacity) * packed_rows + rows % capacity

    row_spots = jnp.concatenate([row_spot + tile * capacity for tile in range(tiles)])
    unpacker = (row_spots[:, None] == spots).astype(jnp.bfloat16)
    flat_rows = jnp.dot(unpacker, received, preferred_element_type=jnp.float32)
    flat_rows = jnp.concatenate(
        [flat_rows[tile * row_count : (tile + 1) * row_count] for tile in range(tiles)], axis=1
    )
    scaled = (flat_rows * SCALE).astype(jnp.float16)
    gathered = lax.all_gather(scaled, "tensor", axis=1, tiled=True)
    accum = jnp.dot(gathered.astype(jnp.bfloat16), up_weight[0], preferred_element_type=jnp.float32)
    hidden = jax.nn.silu(accum * (1.0 / SCALE)).astype(jnp.bfloat16)
    pieces = [hidden, shift(hidden, 1), shift(hidden, -1), leap(hidden)]
    hidden = jnp.concatenate(pieces, axis=1)
    down_mine = jnp.concatenate(down_parts, axis=0)

    def block(k):
        columns = down_mine[:, k * feat : (k + 1) * feat]
        return jnp.dot(hidden, columns, preferred_element_type=jnp.float32)

    half = row_count // 2
    across = block(2).astype(jnp.bfloat16)
    far_one = shift(across[:half], stride)
    far_two = shift(across[half:], -stride)
    ahead, behind = block(1), block(3)
    near_one = shift(ahead[half:].astype(jnp.bfloat16), stride)
    near_two = shift(behind[:half].astype(jnp.bfloat16), -stride)
    keep = block(0)
    sum_one = shift((ahead[:half] + far_one.astype(jnp.float32)).astype(jnp.bfloat16), stride)
    sum_two = shift((behind[half:] + far_two.astype(jnp.float32)).astype(jnp.bfloat16), -stride)
    upper = keep[:half] + near_two.astype(jnp.float32) + sum_one.astype(jnp.float32)
    lower = keep[half:] + near_one.astype(jnp.float32) + sum_two.astype(jnp.float32)
    result = jnp.concatenate([upper, lower], axis=0).astype(jnp.bfloat16)

    stacked = jnp.concatenate(
        [result[:, tile * LANES : (tile + 1) * LANES] for tile in range(tiles)], axis=0
    )
    spot = jnp.arange(experts * packed_rows, dtype=jnp.int32)
    within = spot % packed_rows
    source_row = within // capacity * row_count + spot // packed_rows * capacity + within % capacity
    source_row = jnp.where(within < tiles * capacity, source_row, -1)
    packer = source_row[:, None] == jnp.arange(tiles * row_count, dtype=jnp.int32)[None, :]
    packed = jnp.dot(packer.astype(jnp.bfloat16), stacked, preferred_element_type=jnp.float32)
    packed = packed.astype(jnp.bfloat16).reshape(experts, packed_rows, LANES)
    returned = lax.all_to_all(packed, "dp", split_axis=0, concat_axis=0, tiled=True)
    returned = returned.reshape(experts * packed_rows, LANES)
    spread = jnp.concatenate(
        [jnp.roll(returned, -tile * capacity, axis=0) for tile in range(tiles)], axis=1
    )
    total = 0.0
    for pick in range(picks):
        one_hot = chosen(pick, 0).astype(jnp.bfloat16)
        row = jnp.dot(one_hot, spread, preferred_element_type=jnp.float32)
        total = total + row * combine[:, pick][:, None]
    return with_layout_constraint(total.astype(jnp.bfloat16), Layout(major_to_minor=(0, 1)))


def solution(mesh):
    placed = (
        P("dp", "tensor"),
        P("dp", None),
        P("dp", None),
        P("dp", None, "tensor"),
        P("dp", "tensor", None),
    )
    return jax.shard_map(
        on_device, mesh=mesh, in_specs=placed, out_specs=P("dp", "tensor"), check_vma=False
    )
```

```python
import jax
import jax.numpy as jnp
from jax import lax
from jax.experimental.layout import Layout, with_layout_constraint
from jax.sharding import PartitionSpec as P


LANES = 128
SCALE = 8192.0


GROUPS = 4


def shift(value, step):
    size = lax.axis_size("tensor")
    return lax.ppermute(value, "tensor", [(i, (i + step) % size) for i in range(size)])


def leap(value):
    size = lax.axis_size("tensor")
    pairs = [(i, (i + (2 if i % 2 else -2)) % size) for i in range(size)]
    return lax.ppermute(value, "tensor", pairs)


def on_device(tokens, expert_ids, combine, up_weight, down_weight):
    tok_rows, feat = tokens.shape
    experts = lax.axis_size("dp")
    places = lax.axis_size("tensor")
    stride = places // GROUPS
    capacity = 5 * tok_rows // (2 * experts)
    picks = expert_ids.shape[1]
    tiles = feat // LANES
    packed_rows = -(-(capacity * tiles) // 16) * 16
    row_count = experts * capacity

    down_local = down_weight[0]
    mine = lax.axis_index("tensor")

    def share(move):
        cuts = []
        for turn in range(GROUPS):
            owner = (mine + move + turn * stride + places) % places
            cuts.append(lax.dynamic_slice_in_dim(down_local, owner * feat, feat, axis=1))
        block = jnp.concatenate(cuts, axis=1)
        return with_layout_constraint(block, Layout(major_to_minor=(0, 1)))

    down_parts = [share(0), shift(share(1), 1), shift(share(-1), -1)]
    down_parts.append(leap(share(jnp.where(mine % 2 == 0, -2, 2))))

    token = jnp.arange(tok_rows, dtype=jnp.int32)
    before = token[:, None] < token[None, :]
    slots = []
    for pick in range(picks):
        same = jnp.zeros((tok_rows, tok_rows), jnp.int32)
        for other in range(picks):
            same = same + (expert_ids[:, other][:, None] == expert_ids[:, pick][None, :])
        slots.append(jnp.sum(jnp.where(before, same, 0), axis=0))
    slots = jnp.stack(slots, axis=1)
    place = expert_ids * packed_rows + slots
    spots = jnp.arange(experts * packed_rows, dtype=jnp.int32)[None, :]

    def chosen(pick, tile):
        return place[:, pick][:, None] + tile * capacity == spots

    both = jnp.concatenate([chosen(0, tile) | chosen(1, tile) for tile in range(tiles)], axis=0)
    stacked = jnp.concatenate(
        [tokens[:, tile * LANES : (tile + 1) * LANES] for tile in range(tiles)], axis=0
    )
    outgoing = jnp.einsum(
        "ts,tf->sf", both.astype(jnp.bfloat16), stacked, preferred_element_type=jnp.float32
    )
    outgoing = outgoing.astype(jnp.bfloat16).reshape(experts, packed_rows, LANES)
    received = lax.all_to_all(outgoing, "dp", split_axis=0, concat_axis=0, tiled=True)
    received = received.reshape(experts * packed_rows, LANES)

    rows = jnp.arange(row_count, dtype=jnp.int32)
    row_spot = (rows // capacity) * packed_rows + rows % capacity

    row_spots = jnp.concatenate([row_spot + tile * capacity for tile in range(tiles)])
    unpacker = (row_spots[:, None] == spots).astype(jnp.bfloat16)
    unpacker = lax.optimization_barrier(unpacker)
    flat_rows = jnp.dot(unpacker, received, preferred_element_type=jnp.float32)
    flat_rows = jnp.concatenate(
        [flat_rows[tile * row_count : (tile + 1) * row_count] for tile in range(tiles)], axis=1
    )
    scaled = (flat_rows * SCALE).astype(jnp.float16)
    gathered = lax.all_gather(scaled, "tensor", axis=1, tiled=True)
    accum = jnp.dot(gathered.astype(jnp.bfloat16), up_weight[0], preferred_element_type=jnp.float32)
    hidden = jax.nn.silu(accum * (1.0 / SCALE)).astype(jnp.bfloat16)
    pieces = [hidden, shift(hidden, 1), shift(hidden, -1), leap(hidden)]
    hidden = jnp.concatenate(pieces, axis=1)
    down_mine = jnp.concatenate(down_parts, axis=0)

    def block(k):
        columns = down_mine[:, k * feat : (k + 1) * feat]
        return jnp.dot(hidden, columns, preferred_element_type=jnp.float32)

    half = row_count // 2
    across = block(2).astype(jnp.bfloat16)
    far_one = shift(across[:half], stride)
    far_two = shift(across[half:], -stride)
    ahead, behind = block(1), block(3)
    near_one = shift(ahead[half:].astype(jnp.bfloat16), stride)
    near_two = shift(behind[:half].astype(jnp.bfloat16), -stride)
    keep = block(0)
    sum_one = shift((ahead[:half] + far_one.astype(jnp.float32)).astype(jnp.bfloat16), stride)
    sum_two = shift((behind[half:] + far_two.astype(jnp.float32)).astype(jnp.bfloat16), -stride)
    upper = keep[:half] + near_two.astype(jnp.float32) + sum_one.astype(jnp.float32)
    lower = keep[half:] + near_one.astype(jnp.float32) + sum_two.astype(jnp.float32)
    result = jnp.concatenate([upper, lower], axis=0).astype(jnp.bfloat16)

    stacked = jnp.concatenate(
        [result[:, tile * LANES : (tile + 1) * LANES] for tile in range(tiles)], axis=0
    )
    spot = jnp.arange(experts * packed_rows, dtype=jnp.int32)
    within = spot % packed_rows
    source_row = within // capacity * row_count + spot // packed_rows * capacity + within % capacity
    source_row = jnp.where(within < tiles * capacity, source_row, -1)
    packer = source_row[:, None] == jnp.arange(tiles * row_count, dtype=jnp.int32)[None, :]
    packer = lax.optimization_barrier(packer.astype(jnp.bfloat16))
    packed = jnp.dot(packer, stacked, preferred_element_type=jnp.float32)
    packed = packed.astype(jnp.bfloat16).reshape(experts, packed_rows, LANES)
    returned = lax.all_to_all(packed, "dp", split_axis=0, concat_axis=0, tiled=True)
    returned = returned.reshape(experts * packed_rows, LANES)
    spread = jnp.concatenate(
        [jnp.roll(returned, -tile * capacity, axis=0) for tile in range(tiles)], axis=1
    )
    total = 0.0
    for pick in range(picks):
        one_hot = chosen(pick, 0).astype(jnp.bfloat16)
        row = jnp.dot(one_hot, spread, preferred_element_type=jnp.float32)
        total = total + row * combine[:, pick][:, None]
    return with_layout_constraint(total.astype(jnp.bfloat16), Layout(major_to_minor=(0, 1)))


def solution(mesh):
    placed = (
        P("dp", "tensor"),
        P("dp", None),
        P("dp", None),
        P("dp", None, "tensor"),
        P("dp", "tensor", None),
    )
    return jax.shard_map(
        on_device, mesh=mesh, in_specs=placed, out_specs=P("dp", "tensor"), check_vma=False
    )
```
